256 devices in a mesh: island: 8 (over z_hi, x), row: 8 (over y, core), col: 4 (over z_lo).
Axes of the slice: x: 4, y: 4, z: 8 (z_hi: 2, z_lo: 4; z = z_hi * 4 + z_lo), core: 2. Of those that a mesh axis runs over, the one named last changes fastest.
Arguments:
- deltas: float32 [8, 4096, 8192], P('island', 'row', 'col'), may hold values from -0.26516503 to 0.26516503
- left_stat: float32 [4096, 4096], P(('island', 'col'), 'row'), may hold values from -1.5 to 1.5
- right_stat: float32 [8192, 8192], P(('island', 'row'), 'col'), may hold values from -1.5 to 1.5
Outputs:
- left_new: float32 [4096, 4096], P(('island', 'col'), 'row')
- right_new: float32 [8192, 8192], P(('island', 'row'), 'col')
The draws below stay inside these ranges and needn't reach their ends.
All inputs are finite; a program needn't handle non-finite values.
Results may differ from the reference program's by a relative error of at most 0.00037.
Values may be sent and summed in bfloat16 or wider, within the bound.
No kernel may reach another device: no remote copies, remote signals or barrier semaphores. Data moves between devices by JAX's collectives and lax.ppermute only.
A program may use at most 64 MiB of HBM per device.

```python
import jax
import jax.numpy as jnp
from jax import lax

M = 4096
N = 8192
ISLANDS = 8


def steps_of(own_key, dims, split, smallest, high):
    loudness = 1.0
    for position, shards_of in split:
        draws = jax.random.uniform(jax.random.fold_in(jax.random.fold_in(own_key, 6), position), (shards_of,), jnp.float32, smallest / len(split), high / len(split))
        loudness = loudness * jnp.repeat(jnp.exp(draws), dims[position] // shards_of).reshape((-1,) + (1,) * (len(dims) - 1 - position))
    return loudness


def noise(key, extent, deviation, limit, shards=(), dtype=jnp.bfloat16):
    drawn = jax.random.normal(key, extent, jnp.float32) * deviation
    if len(shards) > 0:
        drawn = steps_of(key, extent, shards, -0.22, 0.18) * drawn
    return jnp.clip(drawn, min=-limit, max=limit).astype(dtype)


def setup_inputs(seed: int = 0) -> dict:
    seeds = jax.random.split(jax.random.key(seed), 4)
    deltas = noise(seeds[0], (ISLANDS, M, N), ((ISLANDS / M) ** 0.5), 0.26516503, ((0, 8), (1, 8), (2, 4)), jnp.float32)
    left_stat = noise(seeds[1], (M, M), 0.25, 1.5, ((0, 32), (1, 8)), jnp.float32)
    right_stat = noise(seeds[2], (N, N), 0.25, 1.5, ((0, 64), (1, 4)), jnp.float32)
    return dict(deltas=deltas, left_stat=left_stat, right_stat=right_stat)


def reference(deltas, left_stat, right_stat):
    outer_grad = jnp.sum(deltas, axis=0) / deltas.shape[0]
    rounded = lax.optimization_barrier(outer_grad.astype(jnp.bfloat16)).astype(jnp.float32)
    left_gram = jnp.dot(rounded, rounded.T, precision=lax.Precision.HIGHEST, preferred_element_type=jnp.float32)
    right_gram = jnp.dot(rounded.T, rounded, precision=lax.Precision.HIGHEST, preferred_element_type=jnp.float32)
    return left_stat + left_gram, right_stat + right_gram
```

```python
import jax
import jax.numpy as jnp
from jax import lax
from jax.sharding import Mesh, PartitionSpec as P

ZH, X, Y, K, C = 2, 4, 4, 2, 4
HALVES = 2
F16 = jnp.float16
F32 = jnp.float32
BF16 = jnp.bfloat16


def shift(n, s):
    return [(i, (i + s) % n) for i in range(n)]


def exchange(block_of, axis, n):
    me = lax.axis_index(axis)
    return [lax.ppermute(block_of((me + s) % n), axis, shift(n, s)) for s in (1, n - 1, *range(2, n - 1))]


def z_routes(chunk):
    table = {
        0: ({1: 0, 3: 4, 5: 6, 4: 2}, {2: (0, 4)[chunk], 7: 6}),
        1: ({0: 1, 4: 3, 6: 7, 3: 5}, {2: 1, 5: (3, 7)[chunk]}),
    }
    routes = []
    for which in range(2):
        pairs = []
        for x in range(X):
            for dst, src in table[x // 2][which].items():
                pairs.append(((src // C * X + x) * C + src % C, (dst // C * X + x) * C + dst % C))
        routes.append(pairs)
    return routes


def y_routes():
    routes = []
    for s in (1, 3, 2):
        pairs = []
        for zh in range(ZH):
            for x in range(X):
                root = 2 * zh + x // 2
                base = (zh * X + x) * Y
                pairs.append((base + root, base + (root + s) % Y))
        routes.append(pairs)
    return routes


def local(deltas, left_stat, right_stat):
    zh, x, y, k, c = (lax.axis_index(a) for a in ("zh", "x", "y", "k", "c"))
    d = deltas[0]
    rows = d.shape[0] // HALVES
    cols = d.shape[1] // X

    sums = []
    for h in range(HALVES):
        chunk = d[h * rows : (h + 1) * rows]

        def block(j, chunk=chunk):
            return (lax.dynamic_slice_in_dim(chunk, j * cols, cols, 1) * 2.0**17).astype(F16)

        own = lax.dynamic_slice_in_dim(chunk, x * cols, cols, 1) * 2.0**17
        for got in exchange(block, "x", X):
            own = own + got.astype(F32)
        sums.append((own * 0.25).astype(F16))
    panels = []
    for h in range(HALVES):
        other = lax.ppermute(sums[h], "zh", shift(ZH, 1))
        total = sums[h].astype(F32) + other.astype(F32)
        rounded = (total * 2.0**-18).astype(BF16)
        coded = (rounded.astype(F32) * 2.0**17).astype(F16)
        panels.append(lax.all_gather(coded, "x", axis=0))

    wanted = 2 * zh + x // 2
    iblk = []
    for h in range(HALVES):
        half = lax.dynamic_slice_in_dim(panels[h], 2 * (x % 2), 2, 0)
        parts = [lax.ppermute(half, ("zh", "x", "c"), route) for route in z_routes(h)]
        iblk.append(jnp.where(c == wanted, half, parts[0] + parts[1]))

    mine, pair = [], []
    for h in range(HALVES):
        keep = lax.dynamic_slice_in_dim(panels[h], 2 * k, 2, 0)
        give = lax.dynamic_slice_in_dim(panels[h], 2 * (1 - k), 2, 0)
        partner = lax.ppermute(give, "k", shift(K, 1))
        pair.append((keep, partner))
        tile = jnp.where(k == x % 2, keep, partner)
        parts = [lax.ppermute(tile, ("zh", "x", "y"), route) for route in y_routes()]
        root = 2 * zh + x // 2
        mine.append(jnp.where(y == root, tile, parts[0] + parts[1] + parts[2]))

    tile = jnp.concatenate(mine, 1).astype(BF16)
    keep = jnp.concatenate([p[0] for p in pair], 1).astype(BF16)
    partner = jnp.concatenate([p[1] for p in pair], 1).astype(BF16)
    dims = (((0, 2), (0, 2)), ((), ()))
    left_keep = lax.dot_general(tile, keep, dims, preferred_element_type=F32)
    left_give = lax.dot_general(tile, partner, dims, preferred_element_type=F32)
    got = lax.ppermute((left_give * 2.0**-26).astype(F16), "k", shift(K, 1))
    left_tile = left_keep * 2.0**-26 + got.astype(F32)
    left_tile = left_tile.reshape(C, -1, left_tile.shape[1])

    def left_block(j):
        return lax.dynamic_index_in_dim(left_tile, j, 0, keepdims=False).astype(F16)

    left = lax.dynamic_index_in_dim(left_tile, c, 0, keepdims=False)
    for got in exchange(left_block, "c", C):
        left = left + got.astype(F32)
    left_new = left_stat + left * 2.0**-8

    columns = jnp.concatenate(iblk, 1).astype(BF16)
    panel = jnp.concatenate(panels, 1).astype(BF16)
    right_tile = jnp.concatenate(
        [
            lax.dot_general(columns, panel[p], (((1,), (0,)), ((), ())), preferred_element_type=F32)
            for p in range(X)
        ],
        2,
    )
    n = right_tile.shape[2]
    right_tile = right_tile.reshape(Y, K, -1, n) * 2.0**-25
    own = lax.dynamic_index_in_dim(right_tile, k, 1, keepdims=False)
    give = lax.dynamic_index_in_dim(right_tile, 1 - k, 1, keepdims=False).astype(F16)
    own = own + lax.ppermute(give, "k", shift(K, 1)).astype(F32)

    def right_block(j):
        return lax.dynamic_index_in_dim(own, j, 0, keepdims=False).astype(F16)

    right = lax.dynamic_index_in_dim(own, y, 0, keepdims=False)
    for got in exchange(right_block, "y", Y):
        right = right + got.astype(F32)
    right_new = right_stat + right * 2.0**-9
    return left_new, right_new


def solution(mesh):
    fine = Mesh(mesh.devices.reshape(ZH, X, Y, K, C), ("zh", "x", "y", "k", "c"))
    i, r, c = ("zh", "x"), ("y", "k"), ("c",)
    specs = (P(i + c, r), P(i + r, c))
    return jax.shard_map(local, mesh=fine, in_specs=(P(i, r, c), *specs), out_specs=specs, check_vma=False)
```

```python
import jax
import jax.numpy as jnp
from jax import lax
from jax.sharding import Mesh, PartitionSpec as P


ZH, X, Y, K, C = 2, 4, 4, 2, 4
HALVES = 2
F16 = jnp.float16
F32 = jnp.float32
BF16 = jnp.bfloat16


def shift(n, s):
    return [(i, (i + s) % n) for i in range(n)]


def exchange(block_of, axis):
    me = lax.axis_index(axis)
    return [lax.ppermute(block_of((me + s) % 4), axis, shift(4, s)) for s in (2, 1, 3)]


def z_routes():
    near = {0: {1: 0, 3: 4, 5: 6, 4: 2}, 1: {0: 1, 4: 3, 6: 7, 3: 5}}
    far = [{0: {2: 0, 7: 6}, 1: {2: 1, 5: 3}}, {0: {2: 4, 7: 6}, 1: {2: 1, 5: 7}}]
    routes = []
    for table in (near, *far):
        pairs = []
        for x in range(X):
            for dst, src in table[x // 2].items():
                pairs.append(((src // C * X + x) * C + src % C, (dst // C * X + x) * C + dst % C))
        routes.append(pairs)
    return routes


def y_route(a, b):
    pairs = []
    for zh in range(ZH):
        for x in range(X):
            base, root, k = (zh * X + x) * Y, 2 * zh + x // 2, x % 2
            pairs.append(((base + (root + a) % Y) * K + k, (base + (root + b) % Y) * K + k))
    return pairs


def local(deltas, left_stat, right_stat):
    zh, x, y, k, c = (lax.axis_index(a) for a in ("zh", "x", "y", "k", "c"))
    d = deltas[0]
    rows = d.shape[0] // HALVES
    cols = d.shape[1] // X

    sums = []
    for h in range(HALVES):

        def block(j, h=h):
            return lax.dynamic_slice(d, (h * rows, j * cols), (rows, cols)) * 2.0**17

        arrived = exchange(lambda j: block(j).astype(F16), "x")
        if h:
            arrived, _ = lax.optimization_barrier((arrived, sums[-1]))
        own = block(x)
        for got in arrived:
            own = own + got.astype(F32)
        sums.append((own * 0.25).astype(F16))
    left_scaled = lax.optimization_barrier(left_stat * 2.0**8)
    panels = []
    for h in range(HALVES):
        other = lax.ppermute(sums[h], "zh", shift(ZH, 1))
        total = sums[h].astype(F32) + other.astype(F32)
        rounded = lax.reduce_precision(total * 2.0**-18, 8, 7)
        panels.append(lax.all_gather((rounded * 2.0**17).astype(F16), "x", axis=1, tiled=True))

    home, side, width = 2 * zh + x // 2, x % 2, cols // 4

    def lanes(block, start, size):
        return lax.dynamic_slice_in_dim(block, start, size, 1)

    near, low, high = z_routes()
    columns, pair = [], []
    for h in range(HALVES):
        part = lanes(panels[h], 2 * cols * side, 2 * cols)
        got = lax.ppermute(part, ("zh", "x", "c"), near)
        if h:
            got += jnp.concatenate(
                [
                    lax.ppermute(part[: rows // 2], ("zh", "x", "c"), low),
                    lax.ppermute(part[rows // 2 :], ("zh", "x", "c"), high),
                ],
                0,
            )
        else:
            got += lax.ppermute(part, ("zh", "x", "c"), low)
        columns.append(jnp.where(c == home, part, got))
        pair.append(lax.ppermute(columns[h], "k", shift(K, 1)))

    def along_y(block, a, b):
        return lax.ppermute(block, ("zh", "x", "y", "k"), y_route(a, b))

    up, down = [along_y(panels[0], 0, 1)], [along_y(panels[1], 0, 3)]
    up.append(along_y(panels[1], 0, 1))
    down.append(along_y(panels[0], 0, 3))
    far = [along_y(up[0], 1, 2), along_y(down[0], 3, 2)]
    tile = []
    for h in range(HALVES):
        tile.append(jnp.where(y == home, lax.optimization_barrier(panels[h]), up[h] + down[1 - h] + far[h]))
    partner = []
    for h in range(HALVES):
        partner.append(lax.ppermute(panels[h], "k", shift(K, 1)))

    panel = [b.astype(BF16) for b in panels]
    panel = jnp.concatenate([*panel, *(b.astype(BF16) for b in partner)], 0)

    half = panel.shape[1] // 2

    def right_blocks(js, side):
        blocks = [
            jnp.concatenate([lanes(b, (2 * j + k) * width, width) for b in (*columns, *pair)], 0).astype(BF16)
            for j in js
        ]
        return lax.dot_general(
            jnp.concatenate(blocks, 1),
            panel[:, side * half : (side + 1) * half],
            (((0,), (0,)), ((), ())),
            preferred_element_type=F32,
        ) * 2.0**-26

    pairings = [(i, i ^ 1) for i in range(Y)], [(i, 3 - i) for i in range(Y)]
    others = y ^ 1, 3 - y
    got = [
        lax.ppermute(right_blocks((others[i], y ^ 2), i).astype(F16), "y", pairings[i]) for i in range(2)
    ]
    kept = [right_blocks((y, others[1 - i]), i) + got[i].astype(F32) for i in range(2)]
    got = [lax.ppermute(kept[i][width:].astype(F16), "y", pairings[1 - i]) for i in range(2)]
    right = jnp.concatenate([kept[i][:width] + got[i].astype(F32) for i in range(2)], 1)
    right_new = right_stat + right * 2.0**-8

    wide = []
    for h in range(HALVES):
        other = lax.ppermute(tile[h], "k", shift(K, 1))
        wide.append(jnp.where(k == side, tile[h], other))
    wide = jnp.concatenate(wide, 0).astype(BF16)
    height = wide.shape[0] // C
    mine = panel[: HALVES * rows]

    def left_block(j):
        return lax.dot_general(
            lax.dynamic_slice_in_dim(wide, j * height, height, 0),
            mine,
            (((1,), (1,)), ((), ())),
            preferred_element_type=F32,
        ) * 2.0**-26

    arrived = exchange(lambda j: left_block(j).astype(F16), "c")
    left = left_block(c)
    for got in arrived:
        left = left + got.astype(F32)
    left_new = (left_scaled + left) * 2.0**-8
    return left_new, right_new


def solution(mesh):
    fine = Mesh(mesh.devices.reshape(ZH, X, Y, K, C), ("zh", "x", "y", "k", "c"))
    i, r, c = ("zh", "x"), ("y", "k"), ("c",)
    specs = (P(i + c, r), P(i + r, c))
    return jax.shard_map(local, mesh=fine, in_specs=(P(i, r, c), *specs), out_specs=specs, check_vma=False)
```

```python
import jax
import jax.numpy as jnp
from jax import lax
from jax.sharding import Mesh, PartitionSpec as P


ZH, X, Y, K, C = 2, 4, 4, 2, 4
HALVES = 2
F16 = jnp.float16
F32 = jnp.float32
BF16 = jnp.bfloat16


def shift(n, s):
    return [(i, (i + s) % n) for i in range(n)]


PAIRINGS = [(i, i ^ 1) for i in range(4)], [(i, 3 - i) for i in range(4)]


def exchange(block_of, axis):
    me = lax.axis_index(axis)
    return [lax.ppermute(block_of((me + s) % 4), axis, shift(4, s)) for s in (2, 1, 3)]


def z_routes():
    near = {0: {1: 0, 3: 4, 5: 6, 4: 2}, 1: {0: 1, 4: 3, 6: 7, 3: 5}}
    far = [{0: {2: 0, 7: 6}, 1: {2: 1, 5: 3}}, {0: {2: 4, 7: 6}, 1: {2: 1, 5: 7}}]
    routes = []
    for table in (near, *far):
        pairs = []
        for x in range(X):
            for dst, src in table[x // 2].items():
                pairs.append(((src // C * X + x) * C + src % C, (dst // C * X + x) * C + dst % C))
        routes.append(pairs)
    return routes


def y_route(a, b):
    pairs = []
    for zh in range(ZH):
        for x in range(X):
            base, root, k = (zh * X + x) * Y, 2 * zh + x // 2, x % 2
            pairs.append(((base + (root + a) % Y) * K + k, (base + (root + b) % Y) * K + k))
    return pairs


def local(deltas, left_stat, right_stat):
    zh, x, y, k, c = (lax.axis_index(a) for a in ("zh", "x", "y", "k", "c"))
    d = deltas[0]
    rows = d.shape[0] // HALVES
    cols = d.shape[1] // X

    sums = []
    for h in range(HALVES):

        def block(j, h=h):
            return lax.dynamic_slice(d, (h * rows, j * cols), (rows, cols)) * 2.0**17

        arrived = exchange(lambda j: block(j).astype(F16), "x")
        if h:
            arrived, _ = lax.optimization_barrier((arrived, sums[-1]))
        own = block(x)
        for got in arrived:
            own = own + got.astype(F32)
        sums.append((own * 0.25).astype(F16))
    quarter = left_stat.shape[0] // 4
    early = lax.optimization_barrier(left_stat[:quarter] * 2.0**8)
    panels = []
    for h in range(HALVES):
        other = lax.ppermute(sums[h], "zh", shift(ZH, 1))
        total = sums[h].astype(F32) + other.astype(F32)
        rounded = (total * 2.0**-18).astype(BF16)
        halves = jnp.split(rounded, 2, 0)
        one = [lax.ppermute(halves[i], "x", PAIRINGS[i]) for i in range(2)]
        two = [jnp.concatenate([one[0], halves[0]], 1), jnp.concatenate([halves[1], one[1]], 1)]
        two = [lax.ppermute(two[i], "x", PAIRINGS[1 - i]) for i in range(2)]
        panels.append(
            lax.optimization_barrier(jnp.concatenate(
                [
                    jnp.concatenate([halves[0], one[0], two[0]], 1),
                    jnp.concatenate([halves[1], two[1], one[1]], 1),
                ],
                0,
            ))
        )

    later, _ = lax.optimization_barrier((left_stat[quarter : 2 * quarter], panels[-1]))
    later = lax.optimization_barrier(later * 2.0**8)
    left_scaled = jnp.concatenate([early, later, left_stat[2 * quarter :] * 2.0**8], 0)

    home, side, width = 2 * zh + x // 2, x % 2, cols // 4

    def lanes(block, start, size):
        return lax.dynamic_slice_in_dim(block, start, size, 1)

    near, low, high = z_routes()
    columns, pair = [], []
    for h in range(HALVES):
        part = lanes(panels[h], 2 * cols * (side ^ (x // 2)), 2 * cols)
        got = lax.ppermute(part, ("zh", "x", "c"), near)
        got += jnp.concatenate(
            [
                lax.ppermute(part[: rows // 2], ("zh", "x", "c"), low),
                lax.ppermute(part[rows // 2 :], ("zh", "x", "c"), high),
            ],
            0,
        )
        columns.append(jnp.where(c == home, part, got))
        pair.append(lax.ppermute(columns[h], "k", shift(K, 1)))

    def along_y(block, a, b):
        return lax.ppermute(block, ("zh", "x", "y", "k"), y_route(a, b))

    up = [along_y(panels[0], 0, 1)]
    down = [along_y(panels[1], 0, 3)]
    up.append(along_y(panels[1], 0, 1))
    down.append(along_y(panels[0], 0, 3))
    far = [along_y(up[0], 1, 2), along_y(down[0], 3, 2)]
    tile = []
    for h in range(HALVES):
        tile.append(jnp.where(y == home, lax.optimization_barrier(panels[h]), up[h] + down[1 - h] + far[h]))
    partner = []
    for h in range(HALVES):
        partner.append(lax.ppermute(panels[h], "k", shift(K, 1)))

    half = panels[0].shape[1] // 2

    def start_of(j):
        return ((j // 2) ^ side) * cols + (j % 2 * K + k) * width

    def right_blocks(js, i):
        total = 0
        for b, panel in zip((*columns, *pair), (*panels, *partner)):
            total += lax.dot_general(
                jnp.concatenate([lanes(b, start_of(j), width) for j in js], 1),
                panel[:, i * half : (i + 1) * half],
                (((0,), (0,)), ((), ())),
                preferred_element_type=F32,
            )
        return total * 2.0**8

    others = y ^ 1, 3 - y
    got = [
        lax.ppermute(right_blocks((others[i], y ^ 2), i).astype(F16), "y", PAIRINGS[i]) for i in range(2)
    ]
    kept = [right_blocks((y, others[1 - i]), i) + got[i].astype(F32) for i in range(2)]
    got = [lax.ppermute(kept[i][width:].astype(F16), "y", PAIRINGS[1 - i]) for i in range(2)]
    right = jnp.concatenate([kept[i][:width] + got[i].astype(F32) for i in range(2)], 1)
    right = jnp.split(right, X, 1)
    right = jnp.concatenate([lax.select_n(x ^ s, *right) for s in range(X)], 1)
    right_new = right_stat + right * 2.0**-8

    wide = []
    for h in range(HALVES):
        other = lax.ppermute(tile[h], "k", shift(K, 1))
        wide.append(jnp.where(k == side, tile[h], other))
    wide = jnp.concatenate(wide, 0)
    height = wide.shape[0] // C

    def left_block(j):
        rows_of = lax.dynamic_slice_in_dim(wide, j * height, height, 0)
        dims = (((1,), (1,)), ((), ()))
        return jnp.concatenate(
            [lax.dot_general(rows_of, b, dims, preferred_element_type=F32) for b in panels], 1
        ) * 2.0**8

    arrived = exchange(lambda j: left_block(j).astype(F16), "c")
    left = left_block(c)
    for got in arrived:
        left = left + got.astype(F32)
    left_new = (left_scaled + left) * 2.0**-8
    return left_new, right_new


def solution(mesh):
    fine = Mesh(mesh.devices.reshape(ZH, X, Y, K, C), ("zh", "x", "y", "k", "c"))
    i, r, c = ("zh", "x"), ("y", "k"), ("c",)
    specs = (P(i + c, r), P(i + r, c))
    return jax.shard_map(local, mesh=fine, in_specs=(P(i, r, c), *specs), out_specs=specs, check_vma=False)
```
